256 devices in a mesh: seq: 64 (over z, x, core), head: 4 (over y).
Axes of the slice: x: 4, y: 4, z: 8, core: 2. Of those that a mesh axis runs over, the one named last changes fastest.
Arguments:
- inputs: bfloat16 [16384, 3072], P('seq'), may hold values from -6 to 6
- decay_logs: float32 [12, 16384], P('head', 'seq'), may hold values from -3 to 0
- query_retain: bfloat16 [3072, 1536], P('seq', 'head'), may hold values from -0.109375 to 0.109375
- key_retain: bfloat16 [3072, 1536], P('seq', 'head'), may hold values from -0.109375 to 0.109375
- value_retain: bfloat16 [3072, 1536], P('seq', 'head'), may hold values from -0.109375 to 0.109375
- output_retain: bfloat16 [3072, 1536], P('seq', 'head'), may hold values from -0.15625 to 0.15625
- key_global: bfloat16 [3072, 512], P('seq', 'head')
- value_global: bfloat16 [3072, 512], P('seq', 'head'), may hold values from -0.109375 to 0.109375
- query_cross: bfloat16 [3072, 1536], P('seq', 'head')
Outputs:
- decoded: float32 [16384, 3072], P('seq')
- attended: bfloat16 [16384, 1536], P('seq', 'head')
The draws below stay inside these ranges and needn't reach their ends.
All inputs are finite; a program needn't handle non-finite values.
Results may differ from the reference program's by a relative error of at most 0.028.
Values may be sent and summed in bfloat16 or wider, within the bound.
No kernel may reach another device: no remote copies, remote signals or barrier semaphores. Data moves between devices by JAX's collectives and lax.ppermute only.
A program may use at most 192 MiB of HBM per device.

```python
import jax
import jax.numpy as jnp
from jax import lax

D = 3072
HD = 128
H_RET = 12
KV_HEADS = 4
Q_CROSS = 12
TOK_DEV = 256
TOKENS = 16384
N_SEQ = 64
N_HEAD = 4


def cross_pair(key):
    asker_generator_init = jax.random.fold_in(key, 101)
    noise_seed = jax.random.fold_in(key, 102)
    queries = jax.random.normal(asker_generator_init, (D, Q_CROSS * HD), jnp.float32) * D ** (-0.5)
    fresh = jax.random.normal(noise_seed, (D, KV_HEADS * HD), jnp.float32) * D ** (-0.5)
    lookup_feature_width = fresh
    return (queries, lookup_feature_width)


def draw_query_cross(key, part):
    return cross_pair(key)[0].astype(jnp.bfloat16)


def draw_key_global(key, part):
    return cross_pair(key)[1].astype(jnp.bfloat16)


def draw_decay_logs(key, part):
    slow_share = 0.5
    slow_mask = jax.random.uniform(jax.random.fold_in(key, 201), (H_RET,), jnp.float32) < slow_share
    slow_rate = jax.random.uniform(jax.random.fold_in(key, 202), (H_RET,), jnp.float32, 0.1, 0.6) / TOKENS
    quick_decay_speed = jax.random.uniform(jax.random.fold_in(key, 203), (H_RET,), jnp.float32, 5.0, 9.0) / TOK_DEV
    decay_rate = jnp.where(slow_mask, slow_rate, quick_decay_speed)
    factor = jnp.exp(jax.random.uniform(jax.random.fold_in(key, 204), (H_RET, TOKENS // TOK_DEV), jnp.float32, jnp.log(0.5), jnp.log(2.0)))
    factor = jnp.repeat(factor, TOK_DEV, axis=1)
    jitter = jax.random.uniform(jax.random.fold_in(key, 205), (H_RET, TOKENS), jnp.float32, 0.5, 1.5)
    settled_period = -decay_rate[:, None] * factor * jitter
    placement_spots = jax.random.randint(jax.random.fold_in(key, 206), (H_RET, 2), 0, TOKENS)
    objective_history = jax.random.uniform(jax.random.fold_in(key, 207), (H_RET, 2), jnp.float32, 0.2, 0.5)
    position = jnp.arange(TOKENS, dtype=jnp.int32)
    agreement_number = (position[None, None, :] == placement_spots[:, :, None]).astype(jnp.float32)
    clustered_bunches = jnp.sum(agreement_number * jnp.log(1.0 - objective_history)[:, :, None], axis=1)
    return jnp.maximum(settled_period + clustered_bunches, -3.0)


def levels(key, dims, shards, smallest, high):
    factor_of, own = 1.0, jax.random.fold_in(key, 6)
    for dim, blocks in shards:
        steps = jnp.exp(jax.random.uniform(jax.random.fold_in(own, dim), (blocks,), jnp.float32, smallest / len(shards), high / len(shards)))
        factor_of = factor_of * jnp.repeat(steps, dims[dim] // blocks).reshape([-1 if axis == dim else 1 for axis in range(len(dims))])
    return factor_of


def gaussian(rng, shape, deviation, bound, pieces=(), kind=jnp.bfloat16):
    array = deviation * jax.random.normal(rng, shape, jnp.float32)
    if pieces:
        array = array * levels(rng, shape, pieces, -0.22, 0.18)
    return jnp.clip(array, -bound, bound).astype(kind)


def setup_inputs(seed: int = 0) -> dict:
    arg_keys = jax.random.split(jax.random.key(seed), 10)
    inputs = gaussian(arg_keys[0], (TOKENS, D), 1.0, 6.0, ((0, 64),))
    decay_logs = draw_decay_logs(jax.random.fold_in(arg_keys[9], 71), 0)
    query_retain = gaussian(arg_keys[2], (D, H_RET * HD), D ** -0.5, 0.109375, ((0, 64), (1, 4)))
    key_retain = gaussian(arg_keys[3], (D, H_RET * HD), D ** -0.5, 0.109375, ((0, 64), (1, 4)))
    value_retain = gaussian(arg_keys[4], (D, H_RET * HD), D ** -0.5, 0.109375, ((0, 64), (1, 4)))
    output_retain = gaussian(arg_keys[5], (D, H_RET * HD), (H_RET * HD) ** -0.5, 0.15625, ((0, 64), (1, 4)))
    key_global = draw_key_global(jax.random.fold_in(arg_keys[9], 71), 0)
    value_global = gaussian(arg_keys[7], (D, KV_HEADS * HD), D ** -0.5, 0.109375, ((0, 64), (1, 4)))
    query_cross = draw_query_cross(jax.random.fold_in(arg_keys[9], 71), 0)
    return dict(inputs=inputs, decay_logs=decay_logs, query_retain=query_retain, key_retain=key_retain, value_retain=value_retain, output_retain=output_retain, key_global=key_global, value_global=value_global, query_cross=query_cross)


def row_norm(values):
    return values * lax.rsqrt(lax.optimization_barrier(jnp.mean(values * values, axis=-1, keepdims=True)) + 1e-06)

def retain_block(carried_state, block_items):
    query_block, key_block, value_block, decay_block = block_items
    running = jnp.cumsum(decay_block, axis=-1)
    length = running.shape[-1]
    causal = jnp.arange(length)[:, None] >= jnp.arange(length)[None, :]
    spread = jnp.where(causal[None], running[:, :, None] - running[:, None, :], 0.0)
    weights = jnp.where(causal[None], jnp.exp(spread), 0.0)
    scores = jnp.einsum('htd,hsd->hts', query_block.astype(jnp.float32), key_block.astype(jnp.float32))
    weighted = (scores * weights).astype(jnp.bfloat16)
    within_block = jnp.einsum('hts,hse->hte', weighted.astype(jnp.float32), value_block.astype(jnp.float32))
    carried = jnp.einsum('htd,hde->hte', query_block.astype(jnp.float32), carried_state, precision=lax.Precision.HIGHEST) * jnp.exp(running)[:, :, None]
    tail_decay = jnp.exp(running[:, -1:] - running)
    faded_keys = (key_block.astype(jnp.float32) * tail_decay[:, :, None]).astype(jnp.bfloat16)
    resident_state = jnp.einsum('htd,hte->hde', faded_keys.astype(jnp.float32), value_block.astype(jnp.float32))
    next_state = jnp.exp(running[:, -1])[:, None, None] * carried_state + resident_state
    return (next_state, within_block + carried)

def reference(inputs, decay_logs, query_retain, key_retain, value_retain, output_retain, key_global, value_global, query_cross):
    input_full = inputs.astype(jnp.float32)
    normed = row_norm(input_full).astype(jnp.bfloat16)

    def by_block(matrix):
        projected = jnp.dot(normed, matrix, preferred_element_type=jnp.float32).astype(jnp.bfloat16)
        return projected.reshape(N_SEQ, TOK_DEV, H_RET, HD).transpose(0, 2, 1, 3)
    decay_blocks = decay_logs.reshape(H_RET, N_SEQ, TOK_DEV).transpose(1, 0, 2)
    start_state = jnp.zeros((H_RET, HD, HD), jnp.float32)
    final_state, outputs = lax.scan(retain_block, start_state, (by_block(query_retain), by_block(key_retain), by_block(value_retain), decay_blocks))
    retained = row_norm(outputs).astype(jnp.bfloat16).transpose(0, 2, 1, 3).reshape(TOKENS, H_RET * HD)
    group_width = H_RET * HD // N_HEAD
    mixed = jnp.zeros((TOKENS, D), jnp.float32)
    for group_index in range(N_HEAD):
        lower = group_index * group_width
        term = jnp.dot(retained[:, lower:lower + group_width], output_retain[:, lower:lower + group_width].T, preferred_element_type=jnp.float32)
        rounded = lax.optimization_barrier(term.astype(jnp.bfloat16))
        mixed = mixed + rounded.astype(jnp.float32)
    decoded = input_full + mixed
    normed_two = row_norm(decoded).astype(jnp.bfloat16)
    key_rows = jnp.dot(normed_two, key_global, preferred_element_type=jnp.float32).astype(jnp.bfloat16)
    value_rows = jnp.dot(normed_two, value_global, preferred_element_type=jnp.float32).astype(jnp.bfloat16)
    cross_queries = (jnp.dot(normed_two, query_cross, preferred_element_type=jnp.float32) * HD ** (-0.5)).astype(jnp.bfloat16)
    group_size = Q_CROSS // KV_HEADS
    key_heads = key_rows.reshape(TOKENS, KV_HEADS, HD).astype(jnp.float32)
    value_heads = value_rows.reshape(TOKENS, KV_HEADS, HD).astype(jnp.float32)
    query_blocks = cross_queries.reshape(N_SEQ, TOK_DEV, KV_HEADS, group_size, HD)
    block_starts = jnp.arange(N_SEQ, dtype=jnp.int32) * TOK_DEV

    def attend(block_items):
        query_block, block_start = block_items
        scores = jnp.einsum('tgqd,sgd->gqts', query_block.astype(jnp.float32), key_heads)
        query_positions = block_start + jnp.arange(TOK_DEV, dtype=jnp.int32)
        allowed = jnp.arange(TOKENS, dtype=jnp.int32)[None, :] <= query_positions[:, None]
        masked = jnp.where(allowed, scores, -1e+30)
        row_top = lax.optimization_barrier(jnp.max(masked, axis=-1, keepdims=True))
        probabilities = jnp.where(allowed, jnp.exp(masked - row_top), 0.0)
        row_total = lax.optimization_barrier(jnp.sum(probabilities, axis=-1))
        rounded = lax.optimization_barrier(probabilities.astype(jnp.bfloat16))
        gathered = jnp.einsum('gqts,sgd->gqtd', rounded.astype(jnp.float32), value_heads)
        result = gathered / row_total[..., None]
        return result.transpose(2, 0, 1, 3).reshape(TOK_DEV, Q_CROSS * HD).astype(jnp.bfloat16)
    attended = lax.map(attend, (query_blocks, block_starts)).reshape(TOKENS, Q_CROSS * HD)
    return (decoded, attended)
```

```python
import functools

import jax
import jax.numpy as jnp
from jax import lax
from jax.experimental import pallas as pl
from jax.experimental.pallas import tpu as pltpu
from jax.sharding import Mesh
from jax.sharding import PartitionSpec as P

HD = 128
Z, X, C, Y = 8, 4, 2, 4
SEQ = ("z", "x", "c")
BF = jnp.bfloat16
F32 = jnp.float32
NEG = -1e30
VMEM = pl.BlockSpec(memory_space=pltpu.VMEM)
SMEM = pl.BlockSpec(memory_space=pltpu.SMEM)


def shifted(array, axis, n, k):
    return lax.ppermute(array, axis, [((i + k) % n, i) for i in range(n)])


def swapped(array):
    return lax.ppermute(array, "c", [(0, 1), (1, 0)])


def row_norm(values):
    return values * lax.rsqrt(jnp.mean(values * values, axis=-1, keepdims=True) + 1e-06)


DX = (0, 1, -1, 2)
DZ_LOW, DZ_HIGH = (0, 1, -1, 2), (-2, 3, -3, 4)
RING = (0, -1, 1, -2, 2, -3, 3, -4)
CROSS = ((0, 0), (-1, 0), (1, 0), (-1, 1), (1, 1), (2, 0), (2, 1), (0, 1))


def routes(dx, dz):
    def place(z, x, c):
        return (z % Z * X + x % X) * C + c

    pairs = []
    for z in range(Z):
        for x in range(X):
            if dz is not None:
                pairs.append((place(z + dz, x, 0), place(z, x, 0)))
            if dx is not None:
                pairs.append((place(z, x + dx, 1), place(z, x, 1)))
    return pairs


def first_routes(dx, dz):
    def place(z, x, c):
        return (z % Z * X + x % X) * C + c

    pairs = []
    for z in range(Z):
        for x in range(X):
            if dx is not None:
                pairs.append((place(z, x + dx, 0), place(z, x, 0)))
            pairs.append((place(z + dz, x, 1), place(z, x, 1)))
    return pairs


def chip_shard(first, half0, half1):
    keep = jnp.where(first, half0, half1)
    other = swapped(jnp.where(first, half1, half0))
    return jnp.concatenate([jnp.where(first, keep, other), jnp.where(first, other, keep)], axis=0)


def spread_near(own):
    got = []
    for i, dz in enumerate((1, -1, 2, -2, 3, -3, 4)):
        got.append(lax.ppermute(own, SEQ, first_routes(DX[i + 1] if i < 3 else None, dz)))
    low = jnp.concatenate([own] + got[:3], axis=0)
    high = jnp.concatenate(got[3:], axis=0)
    return low, high


def spread_far(first, low, high):
    up1 = lax.ppermute(low, SEQ, routes(-1, -1))
    down1 = lax.ppermute(low, SEQ, routes(1, 1))
    up2 = lax.ppermute(jnp.where(first, up1, high), SEQ, routes(-1, -1))
    down2 = lax.ppermute(jnp.where(first, down1, high), SEQ, routes(1, 1))
    up3 = lax.ppermute(jnp.where(first, up2, low), SEQ, routes(2, -1))
    down3 = lax.ppermute(jnp.where(first, down2, high), SEQ, routes(2, 1))
    up4 = lax.ppermute(up3, SEQ, routes(None, -1))
    return (low, up1, down1, up2, down2, up3, down3, up4, high)


def put_rows(place_ref, blocks, out_ref):
    z, x, c = place_ref[0], place_ref[1], place_ref[2]
    first = c == 0
    n = blocks[0].shape[0] // 4
    for r in range(8):
        for s in range(4):
            across, half = CROSS[r]
            dz = jnp.where(first, RING[r], (DZ_LOW, DZ_HIGH)[half][s])
            dx = jnp.where(first, DX[s], across)
            chip = lax.rem(z + dz + Z, Z) * X + lax.rem(x + dx + X, X)
            rows = pl.ds(pl.multiple_of(chip * n, n), n)
            part = slice(s * n, (s + 1) * n)
            if r < 7:
                out_ref[rows, :] = blocks[r][part, :]
            else:
                out_ref[rows, :] = jnp.where(first, blocks[7][part, :], blocks[8][part, :])


def kv_kernel(place_ref, own_ref, other_ref, *refs):
    w_ref = refs[-1]
    put_rows(place_ref, refs[:9], w_ref)
    for x_ref, out_ref in ((own_ref, refs[9]), (other_ref, refs[10])):
        out_ref[...] = jnp.dot(x_ref[...], w_ref[...], preferred_element_type=F32).astype(BF)


def project_pair(place, own, other, blocks):
    width = blocks[0].shape[1]
    out = jax.ShapeDtypeStruct((256, width), BF)
    return pl.pallas_call(
        kv_kernel,
        out_shape=(out, out),
        in_specs=[SMEM] + [VMEM] * 11,
        out_specs=(VMEM, VMEM),
        scratch_shapes=[pltpu.VMEM((3072, width), BF)],
        name="project_pair",
    )(place, own, other, *blocks)


def project_kernel(place_ref, x_ref, a_ref, b_ref, c_ref, d_ref, *refs):
    weights, (dec_ref, q_ref, kv_ref, n_ref) = refs[:5], refs[5:]
    y = place_ref[3]
    for j, piece in enumerate((a_ref, b_ref, c_ref, d_ref)):
        rows = pl.ds(pl.multiple_of(lax.rem(y + j, Y) * 64, 64), 64)
        dec = x_ref[rows, :].astype(F32) + piece[...].astype(F32)
        dec_ref[rows, :] = dec
        n_ref[rows, :] = row_norm(dec).astype(BF)
    w = jnp.concatenate([r[...] for r in weights], axis=1)
    out = jnp.dot(n_ref[...], w, preferred_element_type=F32)
    kv_ref[0:256, :] = out[:, 0:128].astype(BF)
    vt = out[:, 128:256].T.astype(BF)
    kv_ref[256:384, :] = vt[:, 0:128]
    kv_ref[384:512, :] = vt[:, 128:256]
    for h in range(3):
        q_ref[h * 256 : (h + 1) * 256, :] = (out[:, (h + 2) * HD : (h + 3) * HD] * HD ** (-0.5)).astype(BF)


def project(place, inputs, pieces, weights, at):
    def whole(shape):
        return pl.BlockSpec(shape, lambda i: (0, 0))

    def column(k):
        return pl.BlockSpec((3072, HD), lambda i: (0, k))

    return pl.pallas_call(
        project_kernel,
        grid=(1,),
        out_shape=(
            jax.ShapeDtypeStruct((256, 3072), F32),
            jax.ShapeDtypeStruct((768, HD), BF),
            jax.ShapeDtypeStruct((512, HD), BF),
        ),
        in_specs=[SMEM, whole((256, 3072))]
        + [whole((64, 3072))] * 4
        + [column(at // HD + k) for k in range(5)],
        out_specs=(whole((256, 3072)), whole((768, HD)), whole((512, HD))),
        scratch_shapes=[pltpu.VMEM((256, 3072), BF)],
        name="project",
    )(place, inputs, *pieces, *([weights] * 5))


def split_rows(row):
    high = row.astype(BF)
    middle = (row - high.astype(F32)).astype(BF)
    low = (row - high.astype(F32) - middle.astype(F32)).astype(BF)
    return [high, middle, low]


def attend_kernel(steps, first, last, place_ref, q_ref, *refs):
    n = len(steps)
    kv = refs[:n]
    outs = refs[n + (0 if first else 2) :]
    if last:
        own_ref, own_ml_ref, *sent, acc_ref, ml_ref = outs
    else:
        acc_ref, ml_ref = outs
    j = pl.program_id(0)
    z, x, c = place_ref[0], place_ref[1], place_ref[2]
    across = lax.rem(x + j, X)
    if first:
        acc_ref[...] = jnp.zeros_like(acc_ref)
        ml_ref[0, 0:1, :] = jnp.full((1, 768), NEG, F32)
        ml_ref[0, 1:8, :] = jnp.zeros((7, 768), F32)
    else:
        acc_ref[...] = refs[n][...]
        ml_ref[...] = refs[n + 1][...]

    def block(kv_ref, diagonal):
        keys = jnp.concatenate([kv_ref[0, 0:256, :], kv_ref[1, 0:256, :]], axis=0)
        vt = jnp.concatenate([kv_ref[i, k : k + 128, :] for i in range(2) for k in (256, 384)], axis=1)
        if diagonal:
            s_id = lax.broadcasted_iota(jnp.int32, (512, 256), 0)
            t_id = lax.broadcasted_iota(jnp.int32, (512, 256), 1) + 256 * c
            allowed = s_id <= t_id
        spans = [slice(h * 256, (h + 1) * 256) for h in range(3)]
        scores = [
            lax.dot_general(keys, q_ref[0, t, :], (((1,), (1,)), ((), ())), preferred_element_type=F32)
            for t in spans
        ]
        for t, s in zip(spans, scores):
            if diagonal:
                s = jnp.where(allowed, s, NEG)
            old = ml_ref[0, 0:1, t]
            top = jnp.maximum(old, jnp.max(s, axis=0, keepdims=True))
            p = jnp.exp(s - top)
            scale = jnp.exp(old - top)
            ml_ref[0, 0:1, t] = top
            ml_ref[0, 1:2, t] = ml_ref[0, 1:2, t] * scale + jnp.sum(p, axis=0, keepdims=True)
            acc_ref[0, :, t] = acc_ref[0, :, t] * scale + jnp.dot(
                vt, p.astype(BF), preferred_element_type=F32
            )

    for kv_ref, step in zip(kv, steps):
        if step == 0:
            pl.when(across == x)(functools.partial(block, kv_ref, True))
            pl.when(across > x)(functools.partial(block, kv_ref, False))
        else:
            pl.when(lax.rem(z + step + Z, Z) < z)(functools.partial(block, kv_ref, False))

    if last:

        @pl.when(j == 0)
        def _():
            own_ref[...] = acc_ref[0]
            own_ml_ref[...] = ml_ref[0]

        for k, out_ref in enumerate(sent):

            @pl.when(j == k + 1)
            def _(out_ref=out_ref):
                out_ref[0:128, :] = acc_ref[0].astype(BF)
                rows = split_rows(ml_ref[0, 0:1, :]) + split_rows(ml_ref[0, 1:2, :])
                out_ref[128:144, :] = jnp.concatenate(rows + [jnp.zeros((10, 768), BF)], axis=0)


def attend(place, q, kvs, steps, state=None, last=False):
    first = state is None
    acc = jax.ShapeDtypeStruct((4, HD, 768), F32)
    ml = jax.ShapeDtypeStruct((4, 8, 768), F32)
    acc_spec = pl.BlockSpec((1, HD, 768), lambda b: (b, 0, 0))
    ml_spec = pl.BlockSpec((1, 8, 768), lambda b: (b, 0, 0))
    n = len(kvs)
    if last:
        shapes = [((HD, 768), F32), ((8, 768), F32)] + [((144, 768), BF)] * 3
        out_shape = tuple(jax.ShapeDtypeStruct(*s) for s in shapes)
        out_specs = tuple(pl.BlockSpec(s, lambda b: (0, 0)) for s, _ in shapes)
        scratch = [pltpu.VMEM((1, HD, 768), F32), pltpu.VMEM((1, 8, 768), F32)]
    else:
        out_shape, out_specs, scratch = (acc, ml), (acc_spec, ml_spec), []
    return pl.pallas_call(
        functools.partial(attend_kernel, steps, first, last),
        out_shape=out_shape,
        grid=(4,),
        in_specs=[SMEM, pl.BlockSpec((1, 768, HD), lambda b: (b, 0, 0))]
        + [pl.BlockSpec((2, 512, HD), lambda b: (0, 0, 0))] * n
        + ([] if first else [acc_spec, ml_spec]),
        out_specs=out_specs,
        scratch_shapes=scratch,
        input_output_aliases={} if first or last else {2 + n: 0, 3 + n: 1},
        name="attend",
        cost_estimate=pl.CostEstimate(
            flops=4 * 1024 * 384 * 512 * n, transcendentals=1024 * 3 * 512 * n, bytes_accessed=4 << 20
        ),
    )(place, q, *kvs, *(() if first else state))


def finish_kernel(own_ref, ml_ref, *refs):
    out_ref = refs[-1]
    parts = [(own_ref[...], ml_ref[0:1, :], ml_ref[1:2, :])]
    for ref in refs[:-1]:
        stats = ref[128:144, :].astype(F32)
        parts.append(
            (ref[0:128, :].astype(F32), stats[0:1] + stats[1:2] + stats[2:3], stats[3:4] + stats[4:5] + stats[5:6])
        )
    top = functools.reduce(jnp.maximum, [m for _, m, _ in parts])
    scales = [jnp.exp(m - top) for _, m, _ in parts]
    total = sum(l * s for (_, _, l), s in zip(parts, scales))
    result = sum(a * s for (a, _, _), s in zip(parts, scales)) / total
    for h in range(3):
        out_ref[:, h * HD : (h + 1) * HD] = result[:, h * 256 : (h + 1) * 256].T.astype(BF)


def finish(*args):
    return pl.pallas_call(
        finish_kernel,
        out_shape=jax.ShapeDtypeStruct((256, 384), BF),
        in_specs=[VMEM] * 5,
        out_specs=VMEM,
        name="finish",
    )(*args)


def scan_kernel(got_ref, out_ref):
    heads = 3
    decay = got_ref[:, 6, :]
    ones = jnp.ones((1, HD), F32)
    decays = [decay[:, h : h + 1] * ones for h in range(heads)]
    out_ref[...] = jnp.zeros_like(out_ref)
    for h in range(heads):
        rows = slice(2 * h, 2 * h + 2)
        state = jnp.zeros((2, HD), F32)
        for i in range(Z * X):
            out_ref[i, rows, :] = state
            state = decays[h][i : i + 1, :] * state + got_ref[i, rows, :]


def scan_chips(got):
    return pl.pallas_call(
        scan_kernel,
        out_shape=jax.ShapeDtypeStruct(got.shape, F32),
        in_specs=[VMEM],
        out_specs=VMEM,
        name="scan_chips",
    )(got)


def incoming_state(block_decay, other_decay, state, first):
    heads = state.shape[0]
    n = Z * X
    halves = state.reshape(heads, C, HD // C, HD)
    keep = jnp.where(first, halves[:, 0], halves[:, 1])
    other = swapped(jnp.where(first, halves[:, 1], halves[:, 0]))
    core0, core1 = jnp.where(first, keep, other), jnp.where(first, other, keep)
    decay0 = jnp.where(first, block_decay, other_decay)
    decay1 = jnp.where(first, other_decay, block_decay)
    total = decay1[:, None, None] * core0 + core1
    slices = total.reshape(heads, n, HD // C // n, HD).transpose(1, 0, 2, 3).reshape(n, 6, HD)
    row = jnp.pad(decay0 * decay1, (0, HD - heads))[None, None, :]
    sent = jnp.concatenate([slices, jnp.broadcast_to(row, (n, 1, HD)), jnp.zeros((n, 1, HD), F32)], axis=1)
    got = lax.all_to_all(sent, ("z", "x"), 0, 0, tiled=True)
    back = lax.all_to_all(scan_chips(got), ("z", "x"), 0, 0, tiled=True)
    prefix = back[:, :6].reshape(n, heads, 2, HD).transpose(1, 0, 2, 3).reshape(heads, HD // C, HD)
    at1 = decay0[:, None, None] * prefix + core0
    keep = jnp.where(first, prefix, at1)
    other = swapped(jnp.where(first, at1, prefix))
    return jnp.concatenate([jnp.where(first, keep, other), jnp.where(first, other, keep)], axis=1)


def body(inputs, decay_logs, query_retain, key_retain, value_retain, output_retain, key_global, value_global, query_cross):
    z, x, c, y = (lax.axis_index(a) for a in ("z", "x", "c", "head"))
    rows = inputs.shape[0]
    heads = decay_logs.shape[0]
    first = c == 0
    place = jnp.stack([z, x, c, y])
    running = jnp.cumsum(decay_logs, axis=-1)
    block_log = running[:, -1]
    block_decay = jnp.exp(block_log)
    other_decay = swapped(block_decay)
    later = jnp.concatenate([query_retain, output_retain, key_global, value_global, query_cross], axis=1)
    later = lax.all_gather(later, SEQ, axis=0, tiled=True)
    shard_kv = chip_shard(first, key_retain, value_retain)
    low_kv, high_kv = spread_near(shard_kv)
    normed = row_norm(inputs.astype(F32)).astype(BF)
    far_kv = spread_far(first, low_kv, high_kv)
    own_part, other_part = project_pair(place, normed, swapped(normed), far_kv)
    got_part = swapped(other_part)
    width = heads * HD
    q_weights, out_weights = later[:, :width], later[:, width : 2 * width]

    def by_head(matrix):
        return matrix.reshape(rows, heads, HD).transpose(1, 0, 2)

    keys = by_head(jnp.where(first, own_part, got_part))
    values = by_head(jnp.where(first, got_part, own_part))
    tail = jnp.exp(block_log[:, None] - running)
    faded = (keys.astype(F32) * tail[:, :, None]).astype(BF)
    state = jnp.einsum("htd,hte->hde", faded, values, preferred_element_type=F32)
    incoming = incoming_state(block_decay, other_decay, state, first)
    queries = by_head(jnp.dot(normed, q_weights, preferred_element_type=F32).astype(BF))
    causal = (jnp.arange(rows)[:, None] >= jnp.arange(rows)[None, :])[None]
    fade = jnp.where(causal, jnp.exp(jnp.where(causal, running[:, :, None] - running[:, None, :], 0.0)), 0.0)
    scores = jnp.einsum("htd,hsd->hts", queries, keys, preferred_element_type=F32)
    weighted = (scores * fade).astype(BF)
    within = jnp.einsum("hts,hse->hte", weighted, values, preferred_element_type=F32)
    carried = (
        jnp.einsum("htd,hde->hte", queries.astype(F32), incoming, precision=lax.Precision.HIGHEST)
        * jnp.exp(running)[:, :, None]
    )
    retained = row_norm(within + carried).astype(BF).transpose(1, 0, 2).reshape(rows, heads * HD)
    partial = lax.dot_general(
        retained, out_weights, (((1,), (1,)), ((), ())), preferred_element_type=F32
    ).astype(BF)
    terms = lax.all_to_all(partial.reshape(Y, rows // Y, -1), "head", 0, 0, tiled=True)
    mixed = jnp.sum(terms.astype(F32), axis=0).astype(BF)
    pieces = [mixed] + [shifted(mixed, "head", Y, k) for k in (1, 2, 3)]
    decoded, q, kv = project(place, inputs, pieces, later, 2 * width)

    other = swapped(kv)
    kv = jnp.stack([jnp.where(first, kv, other), jnp.where(first, other, kv)])
    q_all = jnp.stack([q] + [shifted(q, "x", X, k) for k in (1, 2, 3)])
    up, down = [kv], [kv]
    for k in range(4):
        up.append(shifted(up[-1], "z", Z, -1))
        if k < 3:
            down.append(shifted(down[-1], "z", Z, 1))
    carry = attend(place, q_all, (kv, up[1], down[1]), (0, -1, 1))
    carry = attend(place, q_all, (up[2], down[2]), (-2, 2), carry)
    own, ml, *parts = attend(place, q_all, (up[3], down[3], up[4]), (-3, 3, -4), carry, last=True)
    attended = finish(own, ml, *[shifted(p, "x", X, -k) for k, p in enumerate(parts, 1)])
    return (decoded, attended)


def solution(mesh):
    split = Mesh(mesh.devices.reshape(Z, X, C, Y), ("z", "x", "c", "head"))
    w = P(SEQ, "head")
    in_specs = (P(SEQ, None), P("head", SEQ)) + (w,) * 7
    out_specs = (P(SEQ, None), P(SEQ, "head"))
    return jax.shard_map(body, mesh=split, in_specs=in_specs, out_specs=out_specs, check_vma=False)
```
